32 devices in a mesh: data: 2 (over x), inner: 4 (over z), stage: 4 (over y, core).
Axes of the slice: x: 2, y: 2, z: 4, core: 2. Of those that a mesh axis runs over, the one named last changes fastest.
Arguments:
- x: bfloat16 [8, 2048, 1024], P(('data', 'stage'), 'inner'), parts along dimension 0
- g: bfloat16 [8, 2048, 1024], P(('data', 'stage'), 'inner'), parts along dimension 0
- w1: bfloat16 [1, 4, 1024, 4096], P(None, 'stage')
- w2: bfloat16 [1, 4, 4096, 1024], P(None, 'stage')
Outputs:
- output 1: bfloat16 [8, 2048, 1024], P(('data', 'stage'), 'inner'), parts along dimension 0
- output 2: bfloat16 [8, 2048, 1024], P(('data', 'stage'), 'inner'), parts along dimension 0
- output 3: float32 [2, 4, 1024, 4096], P('data', 'stage'), parts along dimension 0
- output 4: float32 [2, 4, 4096, 1024], P('data', 'stage'), parts along dimension 0
There are 2 independent parts. The reference program is written for one: setup_inputs(seed, part) draws one part's arguments, and reference() takes and returns one part's arrays. A program takes and returns all parts, laid end to end along the dimension named above; an argument that names none is the same for every part.
All inputs are finite; a program needn't handle non-finite values.
Results may differ from the reference program's by a relative error of at most 0.0126514.
Values are sent between devices in bfloat16 or wider.
A program may use at most 1 GiB of HBM per device.

```python
import jax
import jax.numpy as jnp
from jax import lax

D = 1024
FF = 4096
V = 1
K = 1
STAGE = 4
MICRO = 4
B = 2048

LAYERS = V * STAGE * K


def setup_inputs(seed: int = 0, part: int = 0) -> dict:
    key = jax.random.PRNGKey(seed)
    kbase, kshared = jax.random.split(key)
    kx, kg = jax.random.split(jax.random.fold_in(kbase, part))
    k1, k2 = jax.random.split(kshared)
    x = jax.random.normal(kx, (MICRO, B, D), jnp.float32).astype(jnp.bfloat16)
    g = jax.random.normal(kg, (MICRO, B, D), jnp.float32).astype(jnp.bfloat16)
    w1 = (jax.random.normal(k1, (V, STAGE * K, D, FF), jnp.float32) * D ** -0.5).astype(jnp.bfloat16)
    w2 = (jax.random.normal(k2, (V, STAGE * K, FF, D), jnp.float32) * (2.0 * (FF * LAYERS) ** -0.5)).astype(jnp.bfloat16)
    return {"x": x, "g": g, "w1": w1, "w2": w2}


def _gelu(t):
    return jax.nn.gelu(t, approximate=True)


def _layer_fwd(h, w1, w2):
    z = jnp.dot(h, w1, preferred_element_type=jnp.float32)
    a = _gelu(z).astype(jnp.bfloat16)
    u = jnp.dot(a, w2, preferred_element_type=jnp.float32)
    return (h.astype(jnp.float32) + u).astype(jnp.bfloat16)


def _layer_bwd(h, dh, w1, w2):
    z = jnp.dot(h, w1, preferred_element_type=jnp.float32)
    a32, gelu_vjp = jax.vjp(_gelu, z)
    a = a32.astype(jnp.bfloat16)
    dw2 = jnp.dot(a.T, dh, preferred_element_type=jnp.float32)
    da = jnp.dot(dh, w2.T, preferred_element_type=jnp.float32)
    dz = gelu_vjp(da)[0].astype(jnp.bfloat16)
    dw1 = jnp.dot(h.T, dz, preferred_element_type=jnp.float32)
    dh_prev = (dh.astype(jnp.float32) + jnp.dot(dz, w1.T, preferred_element_type=jnp.float32)).astype(jnp.bfloat16)
    return dh_prev, dw1, dw2


def reference(x, g, w1, w2):
    w1s = w1.reshape(LAYERS, D, FF)
    w2s = w2.reshape(LAYERS, FF, D)

    def one_micro(acc, xg):
        dw1_acc, dw2_acc = acc
        xm, gm = xg

        def fwd(h, w):
            return _layer_fwd(h, w[0], w[1]), h

        y, hs = lax.scan(fwd, xm, (w1s, w2s))

        def bwd(dh, inp):
            h, a, b = inp
            dh_prev, d1, d2 = _layer_bwd(h, dh, a, b)
            return dh_prev, (d1, d2)

        dx, (d1s, d2s) = lax.scan(bwd, gm, (hs, w1s, w2s), reverse=True)
        return (dw1_acc + d1s, dw2_acc + d2s), (y, dx)

    init = (jnp.zeros((LAYERS, D, FF), jnp.float32), jnp.zeros((LAYERS, FF, D), jnp.float32))
    (dw1, dw2), (y, dx) = lax.scan(one_micro, init, (x, g))
    return y, dx, dw1.reshape(w1.shape), dw2.reshape(w2.shape)
```

```python
import functools

import jax
import jax.numpy as jnp
from jax import lax
from jax.experimental import pallas as pl
from jax.experimental.pallas import tpu as pltpu
from jax.sharding import PartitionSpec as P

MESH = pl.DeviceIdType.MESH
F32 = jnp.float32
BF16 = jnp.bfloat16

C = 256
FT = 512
DT = 256
LAG = (11, 8, 4, 1)
X_AT = (0, 0, 4, 4)
G_AT = (0, 8, 8, 16)

C1 = 0.7978845608028654
C2 = 0.044715 * C1


def _gelu_and_slope(z):
    zz = z * z
    s = 0.5 * jnp.tanh(z * (C1 + C2 * zz)) + 0.5
    a = z * s
    slope = s + a * (1.0 - s) * (2.0 * C1 + 6.0 * C2 * zz)
    return a, slope


def _by_stage(p, values):
    out = jnp.int32(values[0])
    for i, v in enumerate(values[1:], 1):
        out = jnp.where(p == i, jnp.int32(v), out)
    return out


def chain_kernel(cfg, x_hbm, g_hbm, w1_hbm, w2_hbm, h_all, g_all, a_all, dz_all, d_all, y_ref, dx_ref,
                 x_ref, g_ref, w1, w2, h_in, g_in, a_st, d_st, d_in, dz_st, h_out, g_out,
                 w_sem, h_sem, g_sem, hl_sem, gl_sem, dl_sem, a_sem, d_sem, dz_sem, hs_sem, gs_sem,
                 xs_sem, gx_sem, y_sem, dx_sem):
    n_stage, n_inner, n, d, f = cfg
    p = lax.axis_index("stage")
    zi = lax.axis_index("inner")
    last = n_stage - 1
    per = n // n_stage
    piece = C // n_inner
    lag = _by_stage(p, LAG)
    x_at = _by_stage(p, X_AT)
    g_at = _by_stage(p, G_AT)

    cx = pltpu.make_async_copy(x_hbm, x_ref, xs_sem)
    cg = pltpu.make_async_copy(g_hbm, g_ref, gx_sem)
    cx.start()
    cg.start()
    cw1 = pltpu.make_async_copy(w1_hbm, w1, w_sem.at[0])
    cw2 = pltpu.make_async_copy(w2_hbm, w2, w_sem.at[1])
    cw1.start()
    cw2.start()

    def hand_out(src, dst, s, sems, send_sem, stage):
        k = p * per + s
        mine = src.at[pl.ds(s * piece, piece), :]
        there = dst.at[k, pl.ds(zi * piece, piece), :]
        for j in range(n_inner):
            here = (p == stage) & (zi == j)

            @pl.when(jnp.logical_not(here))
            def _():
                pltpu.make_async_remote_copy(
                    src_ref=mine, dst_ref=there, send_sem=send_sem, recv_sem=sems.at[k],
                    device_id={"stage": jnp.int32(stage), "inner": jnp.int32(j)}, device_id_type=MESH).start()

            @pl.when(here)
            def _():
                pltpu.make_async_copy(mine, there, sems.at[k]).start()

    def whole(src_slot, dst, k, send_sem, sems, stage):
        return pltpu.make_async_remote_copy(
            src_ref=src_slot, dst_ref=dst.at[k], send_sem=send_sem, recv_sem=sems.at[k],
            device_id={"stage": stage, "inner": zi}, device_id_type=MESH)

    def part(src_slot, dst, k, send_sem, recv_sem, stage, go):
        m, s = lax.div(k, per), lax.rem(k, per)
        mine = src_slot.at[pl.ds(zi * piece, piece), :]
        there = dst.at[pl.ds(s * piece, piece), :]
        if not go:
            pltpu.make_async_copy(mine, there, send_sem).wait()
            return

        @pl.when(m != stage)
        def _():
            pltpu.make_async_remote_copy(
                src_ref=mine, dst_ref=there, send_sem=send_sem, recv_sem=recv_sem,
                device_id={"stage": m, "inner": zi}, device_id_type=MESH).start()

        @pl.when(m == stage)
        def _():
            pltpu.make_async_copy(mine, there, send_sem).start()

    def arrived(buf, sems, k):
        pltpu.make_async_copy(buf.at[k], buf.at[k], sems.at[k]).wait()

    def load_h(k):
        return pltpu.make_async_copy(h_all.at[k], h_in.at[lax.rem(k, 2)], hl_sem.at[lax.rem(k, 2)])

    def load_g(k):
        return pltpu.make_async_copy(g_all.at[k], g_in.at[lax.rem(k, 2)], gl_sem.at[lax.rem(k, 2)])

    def load_d(k):
        return pltpu.make_async_copy(d_all.at[k], d_in, dl_sem)

    def forward(t):
        slot = lax.rem(t, 2)

        load_h(t).wait()
        for j in range(f // FT):
            cols = pl.ds(j * FT, FT)
            z = jnp.dot(h_in[slot], w1[:, cols], preferred_element_type=F32)
            a, slope = _gelu_and_slope(z)
            a_st[:, cols] = a.astype(BF16)
            d_st[:, cols] = slope
        pltpu.make_async_copy(a_st, a_all.at[t], a_sem).start()
        pltpu.make_async_copy(d_st, d_all.at[t], d_sem).start()

        @pl.when(t > 1)
        def _():
            @pl.when(p < last)
            def _():
                whole(h_out.at[slot], h_all, t - 2, hs_sem.at[slot], h_sem, p + 1).wait_send()

            @pl.when(p == last)
            def _():
                part(h_out.at[slot], y_ref, t - 2, hs_sem.at[slot], y_sem, last, False)

        for j in range(d // DT):
            cols = pl.ds(j * DT, DT)
            u = jnp.dot(a_st[...], w2[:, cols], preferred_element_type=F32)
            h_out[slot, :, cols] = (h_in[slot, :, cols].astype(F32) + u).astype(BF16)

        @pl.when(p < last)
        def _():
            whole(h_out.at[slot], h_all, t, hs_sem.at[slot], h_sem, p + 1).start()

        @pl.when(p == last)
        def _():
            part(h_out.at[slot], y_ref, t, hs_sem.at[slot], y_sem, last, True)

    def backward(k):
        slot = lax.rem(k, 2)

        @pl.when(k > 0)
        def _():
            pltpu.make_async_copy(dz_st, dz_all.at[k - 1], dz_sem).wait()

        load_g(k).wait()
        load_d(k).wait()
        nt = (((1,), (1,)), ((), ()))
        for j in range(f // FT):
            cols = pl.ds(j * FT, FT)
            da = lax.dot_general(g_in[slot], w2[cols, :], nt, preferred_element_type=F32)
            dz_st[:, cols] = (da * d_in[:, cols]).astype(BF16)
        pltpu.make_async_copy(dz_st, dz_all.at[k], dz_sem).start()

        @pl.when(k > 1)
        def _():
            @pl.when(p > 0)
            def _():
                whole(g_out.at[slot], g_all, k - 2, gs_sem.at[slot], g_sem, p - 1).wait_send()

            @pl.when(p == 0)
            def _():
                part(g_out.at[slot], dx_ref, k - 2, gs_sem.at[slot], dx_sem, 0, False)

        for j in range(d // DT):
            cols = pl.ds(j * DT, DT)
            dh = lax.dot_general(dz_st[...], w1[cols, :], nt, preferred_element_type=F32)
            g_out[slot, :, cols] = (g_in[slot, :, cols].astype(F32) + dh).astype(BF16)

        @pl.when(p > 0)
        def _():
            whole(g_out.at[slot], g_all, k, gs_sem.at[slot], g_sem, p - 1).start()

        @pl.when(p == 0)
        def _():
            part(g_out.at[slot], dx_ref, k, gs_sem.at[slot], dx_sem, 0, True)

    cx.wait()
    cg.wait()

    @pl.when(p == 0)
    def _():
        for s in range(per):
            hand_out(x_ref, h_all, s, h_sem, xs_sem, 0)

    def step(t, _):
        kb = t - lag
        do_f = t < n
        do_b = (kb >= 0) & (kb < n)
        sx = t - x_at
        sg = t - g_at

        @pl.when((t > 0) & (t <= n))
        def _():
            pltpu.make_async_copy(a_st, a_all.at[t - 1], a_sem).wait()
            pltpu.make_async_copy(d_st, d_all.at[t - 1], d_sem).wait()

        @pl.when((p > 0) & (sx >= 0) & (sx < per))
        def _():
            hand_out(x_ref, h_all, sx, h_sem, xs_sem, 0)

        @pl.when((sg >= 0) & (sg < per))
        def _():
            hand_out(g_ref, g_all, sg, g_sem, gx_sem, last)

        @pl.when(t == 0)
        def _():
            arrived(h_all, h_sem, t)
            load_h(t).start()
            cw1.wait()
            cw2.wait()

        @pl.when(do_b)
        def _():
            arrived(g_all, g_sem, kb)
            load_g(kb).start()

        @pl.when(do_b & (t < n))
        def _():
            load_d(kb).start()

        @pl.when(do_f)
        def _():
            forward(t)

        @pl.when(do_b & (t >= n))
        def _():
            load_d(kb).start()

        @pl.when(t + 1 < n)
        def _():
            arrived(h_all, h_sem, t + 1)
            load_h(t + 1).start()

        @pl.when(do_b)
        def _():
            backward(kb)

        return 0

    lax.fori_loop(0, n + max(LAG), step, 0)

    pltpu.make_async_copy(dz_st, dz_all.at[n - 1], dz_sem).wait()
    for k in (n - 2, n - 1):
        slot = k % 2

        @pl.when(p < last)
        def _():
            whole(h_out.at[slot], h_all, k, hs_sem.at[slot], h_sem, p + 1).wait_send()

        @pl.when(p == last)
        def _():
            part(h_out.at[slot], y_ref, jnp.int32(k), hs_sem.at[slot], y_sem, last, False)

        @pl.when(p > 0)
        def _():
            whole(g_out.at[slot], g_all, k, gs_sem.at[slot], g_sem, p - 1).wait_send()

        @pl.when(p == 0)
        def _():
            part(g_out.at[slot], dx_ref, jnp.int32(k), gs_sem.at[slot], dx_sem, 0, False)

    full = n // n_stage
    less = full * (n_inner - 1) // n_inner
    for buf, sem, stage, out, out_sem, out_stage in (
        (h_all, xs_sem, 0, y_ref, y_sem, last), (g_all, gx_sem, last, dx_ref, dx_sem, 0)):
        @pl.when(p != stage)
        def _():
            pltpu.make_async_copy(buf.at[pl.ds(0, full)], buf.at[pl.ds(0, full)], sem).wait()

        @pl.when(p == stage)
        def _():
            pltpu.make_async_copy(buf.at[pl.ds(0, less)], buf.at[pl.ds(0, less)], sem).wait()

        @pl.when(p != out_stage)
        def _():
            pltpu.make_async_copy(out, out, out_sem).wait()


def chain(cfg, x, g, w1, w2):
    n_stage, n_inner, n, d, f = cfg
    any_ = pl.BlockSpec(memory_space=pl.ANY)
    rows = x.shape[0]
    shape = jax.ShapeDtypeStruct
    dma = pltpu.SemaphoreType.DMA
    return pl.pallas_call(
        functools.partial(chain_kernel, cfg),
        name="chain",
        out_shape=(
            shape((n, C, d), BF16), shape((n, C, d), BF16), shape((n, C, f), BF16), shape((n, C, f), BF16),
            shape((n, C, f), F32), shape((rows, d), BF16), shape((rows, d), BF16),
        ),
        in_specs=[any_] * 4,
        out_specs=(any_,) * 7,
        scratch_shapes=[
            pltpu.VMEM((rows, d), BF16), pltpu.VMEM((rows, d), BF16), pltpu.VMEM((d, f), BF16), pltpu.VMEM((f, d), BF16),
            pltpu.VMEM((2, C, d), BF16), pltpu.VMEM((2, C, d), BF16),
            pltpu.VMEM((C, f), BF16), pltpu.VMEM((C, f), F32), pltpu.VMEM((C, f), F32), pltpu.VMEM((C, f), BF16),
            pltpu.VMEM((2, C, d), BF16), pltpu.VMEM((2, C, d), BF16),
            dma((2,)), dma((n,)), dma((n,)), dma((2,)), dma((2,)), dma, dma, dma, dma, dma((2,)), dma((2,)),
            dma, dma, dma, dma,
        ],
        compiler_params=pltpu.CompilerParams(has_side_effects=True, vmem_limit_bytes=60 * 2**20),
        cost_estimate=pl.CostEstimate(
            flops=8 * n * C * d * f, bytes_accessed=n * C * (f * 14 + d * 8), transcendentals=n * C * f),
    )(x, g, w1, w2)


def solution(mesh):
    n_stage, n_inner = mesh.shape["stage"], mesh.shape["inner"]

    def body(x, g, w1, w2):
        _, rows, d = x.shape
        f = w1.shape[-1]
        n = rows * n_inner * n_stage // C
        cfg = (n_stage, n_inner, n, d, f)
        h_all, g_all, a_all, dz_all, _, y, dx = chain(
            cfg, x.reshape(rows, d), g.reshape(rows, d), w1.reshape(d, f), w2.reshape(f, d))
        tn = (((0,), (0,)), ((), ()))
        h2, g2 = h_all.reshape(n * C, d), g_all.reshape(n * C, d)
        dw1 = lax.dot_general(h2, dz_all.reshape(n * C, f), tn, preferred_element_type=F32)
        dw2 = lax.dot_general(a_all.reshape(n * C, f), g2, tn, preferred_element_type=F32)
        return y.reshape(x.shape), dx.reshape(g.shape), dw1.reshape(1, 1, d, f), dw2.reshape(1, 1, f, d)

    tok = P(("data", "stage"), "inner", None)
    wsp = P(None, "stage", None, None)
    dsp = P("data", "stage", None, None)
    return jax.shard_map(body, mesh=mesh, in_specs=(tok, tok, wsp, wsp), out_specs=(tok, tok, dsp, dsp), check_vma=False)
```
